32 devices in a mesh: ha: 8 (over z, core), wa: 2 (over y), ba: 2 (over x).
Axes of the slice: x: 2, y: 2, z: 4, core: 2. Of those that a mesh axis runs over, the one named last changes fastest.
Arguments:
- tokens: bfloat16 [2, 128, 64, 384], P('ba', 'ha', 'wa'), may hold values from -6 to 6
- cotangent: bfloat16 [2, 128, 64, 384], P('ba', 'ha', 'wa'), may hold values from -6 to 6
- w_qkv: bfloat16 [384, 1152], replicated, may hold values from -0.20412415 to 0.20412415
- w_proj: bfloat16 [384, 384], replicated, may hold values from -0.3125 to 0.3125
- table_logits: float32 [12, 225], replicated, may hold values from -6 to 6
- logit_scale: float32 [12], replicated, may hold values from 1 to 5.5
- gain: float32 [384], replicated, may hold values from 0.5 to 1.5
Outputs:
- d_tokens: bfloat16 [2, 128, 64, 384], P('ba', 'ha', 'wa')
- d_wqkv: float32 [384, 1152], P(None, 'ba')
- d_wproj: float32 [384, 384], P(None, 'ba')
- d_table: float32 [12, 225], replicated
- d_scale: float32 [12], replicated
- d_gain: float32 [384], replicated
The draws below stay inside these ranges and needn't reach their ends.
All inputs are finite; a program needn't handle non-finite values.
Results may differ from the reference program's by a relative error of at most 0.01.
The reference program's roundings to bfloat16 on the way count: a program that leaves them out, or rounds other values in their place, can miss the bound.
Values may be sent and summed in bfloat16 or wider, within the bound.
A program may use at most 64 MiB of HBM per device.

```python
import math
import jax
import jax.numpy as jnp
from jax import lax

HEADS = 12
C = 384
WIN = 8
TABLE = 225
HEIGHT = 128
WIDTH = 64
BATCH = 2


def draw_w_qkv(key, part):
    spread = C ** (-0.5)
    base = jax.random.normal(key, (C, 3 * C), jnp.float32) * spread
    base = jnp.clip(base, -4.0 * spread, 4.0 * spread)
    return base.astype(jnp.bfloat16)


def shard_levels(key, shape, cuts, low, largest):
    factor_of, own = 1.0, jax.random.fold_in(key, 6)
    for dim, shards_of in cuts:
        heights = jnp.exp(jax.random.uniform(jax.random.fold_in(own, dim), (shards_of,), jnp.float32, low / len(cuts), largest / len(cuts)))
        factor_of = factor_of * jnp.repeat(heights, shape[dim] // shards_of).reshape([-1 if axis == dim else 1 for axis in range(len(shape))])
    return factor_of


def normal_values(own_key, shape, deviation, most, shards=(), kind=jnp.bfloat16):
    values = jax.random.normal(own_key, shape, jnp.float32) * deviation
    if len(shards) > 0:
        values = shard_levels(own_key, shape, shards, -0.22, 0.18) * values
    return jnp.clip(values, min=-most, max=most).astype(kind)


def setup_inputs(seed: int = 0) -> dict:
    splits = jax.random.split(jax.random.key(seed), 8)
    return {
        "tokens": normal_values(splits[0], (BATCH, HEIGHT, WIDTH, C), 1.0, 6.0, ((0, 2), (1, 8), (2, 2))),
        "cotangent": normal_values(splits[1], (BATCH, HEIGHT, WIDTH, C), 1.0, 6.0, ((0, 2), (1, 8), (2, 2))),
        "w_qkv": draw_w_qkv(jax.random.fold_in(splits[7], 71), 0),
        "w_proj": normal_values(splits[3], (C, C), C ** -0.5, 0.3125),
        "table_logits": normal_values(splits[4], (HEADS, TABLE), 1.5, 6.0, (), jnp.float32),
        "logit_scale": jnp.clip(jax.random.uniform(splits[5], (HEADS,), jnp.float32, 1.0, 5.5), 1.0, 5.5),
        "gain": jnp.clip(1.0 + 0.1 * jax.random.normal(splits[6], (C,), jnp.float32), 0.5, 1.5),
    }


EPS_NORM = 1e-05
MASK_FILL = -100.0
SCALE_CAP = math.log(100.0)
BIAS_RANGE = 16.0
HIGHEST = lax.Precision.HIGHEST

def coarse_product(form, left, right):
    return jnp.einsum(form, left.astype(jnp.float32), right.astype(jnp.float32), precision=HIGHEST)

def fine_product(form, left, right):
    return jnp.einsum(form, left, right, precision=HIGHEST)

def to_windows(block, window):
    images, height, width, depth = block.shape
    tiles = block.reshape(images, height // window, window, width // window, window, depth)
    tiles = tiles.transpose(0, 1, 3, 2, 4, 5)
    return tiles.reshape(images, height // window * (width // window), window * window, depth)

def from_windows(tiles, images, height, width, window):
    depth = tiles.shape[-1]
    grid = tiles.reshape(images, height // window, width // window, window, window, depth)
    return grid.transpose(0, 1, 3, 2, 4, 5).reshape(images, height, width, depth)

def position_onehot(window):
    places = jnp.arange(window * window, dtype=jnp.int32)
    row_of = places // window
    col_of = places % window
    offset = (row_of[:, None] - row_of[None, :] + window - 1) * (2 * window - 1) + (col_of[:, None] - col_of[None, :] + window - 1)
    entries = jnp.arange((2 * window - 1) ** 2, dtype=jnp.int32)
    return (offset.reshape(-1)[:, None] == entries[None, :]).astype(jnp.float32)

def region_of(coords, extent, window):
    return (coords >= extent - window).astype(jnp.int32) + (coords >= extent - window // 2).astype(jnp.int32)

def region_mask(row_start, col_start, rows, cols, height, width, window):
    row_label = region_of(row_start + jnp.arange(rows, dtype=jnp.int32), height, window)
    col_label = region_of(col_start + jnp.arange(cols, dtype=jnp.int32), width, window)
    labels = row_label[:, None] * 3 + col_label[None, :]
    labels = labels.reshape(rows // window, window, cols // window, window).transpose(0, 2, 1, 3)
    labels = labels.reshape(-1, window * window)
    return jnp.where(labels[:, :, None] != labels[:, None, :], MASK_FILL, 0.0).astype(jnp.float32)

def grads_region(block, grad_block, row_start, col_start, height, width, window, params):
    w_qkv, w_proj, table_logits, logit_scale, gain = params
    images, rows, cols, depth = block.shape
    heads = logit_scale.shape[0]
    head_dim = depth // heads
    tiles = to_windows(block, window)
    grad_tiles = to_windows(grad_block, window)
    count = tiles.shape[1]
    length = window * window
    flat = tiles.reshape(-1, depth)
    qkv = jnp.dot(flat, w_qkv, preferred_element_type=jnp.float32).astype(jnp.bfloat16)
    qkv = qkv.reshape(images, count, length, 3, heads, head_dim)
    query = qkv[:, :, :, 0].astype(jnp.float32)
    keys = qkv[:, :, :, 1].astype(jnp.float32)
    values = qkv[:, :, :, 2]
    query_inv = lax.rsqrt(lax.optimization_barrier(jnp.sum(query * query, -1, keepdims=True)) + 1.0)
    key_inv = lax.rsqrt(lax.optimization_barrier(jnp.sum(keys * keys, -1, keepdims=True)) + 1.0)
    unit_query = query * query_inv
    unit_key = keys * key_inv
    scale = jnp.exp(jnp.minimum(logit_scale, SCALE_CAP))
    onehot = position_onehot(window)
    sigma = jax.nn.sigmoid(table_logits)
    rel_bias = jnp.dot(sigma * BIAS_RANGE, onehot.T, precision=HIGHEST).reshape(heads, length, length)
    mask = region_mask(row_start, col_start, rows, cols, height, width, window)
    cosine = fine_product('bnqhd,bnkhd->bnhqk', unit_query, unit_key)
    scores = scale[:, None, None] * cosine + rel_bias[None, None] + mask[None, :, None]
    top = lax.optimization_barrier(jnp.max(scores, -1, keepdims=True))
    expo = jnp.exp(scores - top)
    probs = expo / lax.optimization_barrier(jnp.sum(expo, -1, keepdims=True))
    probs_low = probs.astype(jnp.bfloat16)
    attended = coarse_product('bnhqk,bnkhd->bnqhd', probs_low, values).astype(jnp.bfloat16).reshape(-1, depth)
    proj = jnp.dot(attended, w_proj, preferred_element_type=jnp.float32)
    centre = proj - lax.optimization_barrier(jnp.mean(proj, -1, keepdims=True))
    inv_std = lax.rsqrt(lax.optimization_barrier(jnp.mean(centre * centre, -1, keepdims=True)) + EPS_NORM)
    normed = centre * inv_std
    upstream = grad_tiles.reshape(-1, depth).astype(jnp.float32)
    d_gain = lax.optimization_barrier(jnp.sum(upstream * normed, 0))
    scaled = upstream * gain
    d_proj = inv_std * (scaled - lax.optimization_barrier(jnp.mean(scaled, -1, keepdims=True)) - normed * lax.optimization_barrier(jnp.mean(scaled * normed, -1, keepdims=True)))
    d_proj = d_proj.astype(jnp.bfloat16)
    d_wproj = jnp.dot(attended.T, d_proj, preferred_element_type=jnp.float32)
    d_att = jnp.dot(d_proj, w_proj.T, preferred_element_type=jnp.float32).astype(jnp.bfloat16)
    d_att = d_att.reshape(images, count, length, heads, head_dim)
    d_probs = coarse_product('bnqhd,bnkhd->bnhqk', d_att, values)
    d_values = coarse_product('bnhqk,bnqhd->bnkhd', probs_low, d_att)
    d_scores = probs * (d_probs - lax.optimization_barrier(jnp.sum(d_probs * probs, -1, keepdims=True)))
    d_bias = lax.optimization_barrier(jnp.sum(d_scores, (0, 1))).reshape(heads, length * length)
    d_table = jnp.dot(d_bias, onehot, precision=HIGHEST) * (BIAS_RANGE * sigma * (1.0 - sigma))
    live = (logit_scale < SCALE_CAP).astype(jnp.float32)
    d_scale = lax.optimization_barrier(jnp.sum(d_scores * cosine, (0, 1, 3, 4))) * scale * live
    d_cos = d_scores * scale[:, None, None]
    d_unit_q = fine_product('bnhqk,bnkhd->bnqhd', d_cos, unit_key)
    d_unit_k = fine_product('bnhqk,bnqhd->bnkhd', d_cos, unit_query)
    d_query = query_inv * (d_unit_q - unit_query * lax.optimization_barrier(jnp.sum(unit_query * d_unit_q, -1, keepdims=True)))
    d_key = key_inv * (d_unit_k - unit_key * lax.optimization_barrier(jnp.sum(unit_key * d_unit_k, -1, keepdims=True)))
    d_qkv = jnp.stack([d_query, d_key, d_values], 3).astype(jnp.bfloat16).reshape(-1, 3 * depth)
    d_wqkv = jnp.dot(flat.T, d_qkv, preferred_element_type=jnp.float32)
    d_flat = jnp.dot(d_qkv, w_qkv.T, preferred_element_type=jnp.float32).astype(jnp.bfloat16)
    d_block = from_windows(d_flat.reshape(images, count, length, depth), images, rows, cols, window)
    return (d_block, (d_wqkv, d_wproj, d_table, d_scale, d_gain))

def reference(tokens, cotangent, w_qkv, w_proj, table_logits, logit_scale, gain):
    shift = WIN // 2
    images, height, width, depth = tokens.shape
    moved = jnp.roll(tokens, (-shift, -shift), axis=(1, 2))
    moved_grad = jnp.roll(cotangent, (-shift, -shift), axis=(1, 2))
    params = (w_qkv, w_proj, table_logits, logit_scale, gain)
    bands = height // WIN
    anchor = jnp.zeros((), jnp.int32)

    def one_band(totals, index):
        image = (index // bands).astype(jnp.int32)
        start = (index % bands * WIN).astype(jnp.int32)
        block = lax.dynamic_slice(moved, (image, start, anchor, anchor), (1, WIN, width, depth))
        grad_block = lax.dynamic_slice(moved_grad, (image, start, anchor, anchor), (1, WIN, width, depth))
        d_block, parts = grads_region(block, grad_block, start, anchor, height, width, WIN, params)
        return (jax.tree.map(jnp.add, totals, parts), d_block[0])
    initial = (jnp.zeros((depth, 3 * depth), jnp.float32), jnp.zeros((depth, depth), jnp.float32), jnp.zeros(table_logits.shape, jnp.float32), jnp.zeros(logit_scale.shape, jnp.float32), jnp.zeros(gain.shape, jnp.float32))
    totals, pieces = lax.scan(one_band, initial, jnp.arange(images * bands, dtype=jnp.int32))
    d_moved = pieces.reshape(images, height, width, depth)
    back = jnp.roll(d_moved, (shift, shift), axis=(1, 2))
    d_tokens = (cotangent.astype(jnp.float32) + back.astype(jnp.float32)).astype(jnp.bfloat16)
    return (d_tokens, totals[0], totals[1], totals[2], totals[3], totals[4])
```

```python
import math

import functools

import jax
import jax.numpy as jnp
import numpy as np
from jax import lax
from jax.experimental import pallas as pl
from jax.experimental.pallas import tpu as pltpu
from jax.sharding import PartitionSpec as P

WIN = 8


EPS_NORM = 1e-05
MASK_FILL = -100.0
SCALE_CAP = math.log(100.0)
BIAS_RANGE = 16.0


def from_behind(block, axis, distance):
    devices = range(lax.axis_size(axis))
    route = [((i - distance) % len(devices), i) for i in devices]
    return lax.ppermute(block, axis, route)


def to_windows(block, window):
    images, height, width, depth = block.shape
    tiles = block.reshape(images, height // window, window, width // window, window, depth)
    tiles = tiles.transpose(0, 1, 3, 2, 4, 5)
    return tiles.reshape(images, height // window * (width // window), window * window, depth)


def from_windows(tiles, images, height, width, window):
    depth = tiles.shape[-1]
    grid = tiles.reshape(images, height // window, width // window, window, window, depth)
    return grid.transpose(0, 1, 3, 2, 4, 5).reshape(images, height, width, depth)


def region_of(coords, extent, window):
    return (coords >= extent - window).astype(jnp.int32) + (coords >= extent - window // 2).astype(
        jnp.int32
    )

GROUP = 4
MESH = pl.DeviceIdType.MESH
VMEM = pl.BlockSpec(memory_space=pltpu.VMEM)
NN = (((1,), (0,)), ((), ()))
NT = (((1,), (1,)), ((), ()))
TN = (((0,), (0,)), ((), ()))


def mxu(left, right, dims):
    return lax.dot_general(left, right, dims, preferred_element_type=jnp.float32)


def split(value):
    high = value.astype(jnp.bfloat16)
    return high, (value - high.astype(jnp.float32)).astype(jnp.bfloat16)


def mxu_fine(left, right, dims):
    high, low = split(left)
    return mxu(high, right, dims) + mxu(low, right, dims)


def same_block(rows, cols, row_size, col_size):
    row = lax.broadcasted_iota(jnp.int32, (rows, cols), 0) // row_size
    col = lax.broadcasted_iota(jnp.int32, (rows, cols), 1) // col_size
    return (row == col).astype(jnp.bfloat16)


def spread(value, width, length):
    tall = jnp.concatenate([value] * GROUP, 0)
    return tall * same_block(tall.shape[0], tall.shape[1], length, width)


def gather_heads(value, width, length):
    lane = lax.broadcasted_iota(jnp.int32, (length, value.shape[1]), 1) // width
    total = jnp.where(lane == 0, value[:length], 0.0)
    for head in range(1, GROUP):
        total = jnp.where(lane == head, value[head * length : (head + 1) * length], total)
    return total


def segment_max(value, size):
    lane = lax.broadcasted_iota(jnp.int32, value.shape, 1) // size
    top = jnp.zeros_like(value)
    for head in range(value.shape[1] // size):
        here = jnp.max(jnp.where(lane == head, value, -jnp.inf), -1, keepdims=True)
        top = jnp.where(lane == head, here, top)
    return top


def local_kernel(
    grid_cols, height, width, window,
    flat_ref, grad_ref, w_qkv_ref, w_proj_ref, bias_ref, scale_ref, gain_ref,
    d_flat_ref, d_wqkv_ref, d_wproj_ref, d_bias_ref, d_cos_ref, d_gain_ref,
    qkv_ref, att_ref, d_att_ref, d_qkv_ref, probs_ref, cos_ref,
):
    tokens, depth = flat_ref.shape
    length = window * window
    count = tokens // length
    groups = bias_ref.shape[0]
    lanes = depth // groups
    head_dim = lanes // GROUP
    wide = GROUP * length
    row_base = lax.axis_index("ha") * (count // grid_cols * window)
    col_base = lax.axis_index("wa") * (grid_cols * window)

    qkv_ref[...] = mxu(flat_ref[...], w_qkv_ref[...], NN).astype(jnp.bfloat16)
    lane_ones = same_block(lanes, wide, head_dim, length)
    wide_ones = same_block(wide, wide, length, length)
    lane_lane = same_block(lanes, lanes, head_dim, head_dim)
    row_ones = jnp.ones((8, lanes), jnp.bfloat16)

    def labels(place, first_row, first_col):
        place = place % length
        row = first_row + place // window
        col = first_col + place % window
        return region_of(row, height, window) * 3 + region_of(col, width, window)

    def load(w, g, part):
        return qkv_ref[
            pl.ds(pl.multiple_of(w * length, length), length),
            part * depth + g * lanes : part * depth + (g + 1) * lanes,
        ]

    def key_row_inv(tall):
        high, low = split(jnp.square(tall.astype(jnp.float32)))
        total = mxu(row_ones, high, NT) + mxu(row_ones, low, NT)
        return lax.rsqrt(total[:1] + 1.0)

    def forward(w, carry):
        first_row = row_base + w // grid_cols * window
        first_col = col_base + w % grid_cols * window
        shape = (length, wide)
        mine = labels(lax.broadcasted_iota(jnp.int32, shape, 0), first_row, first_col)
        other = labels(lax.broadcasted_iota(jnp.int32, shape, 1), first_row, first_col)
        mask = jnp.where(mine != other, MASK_FILL, 0.0)
        for g in range(groups):
            query, key, value = load(w, g, 0), load(w, g, 1), load(w, g, 2)
            tall = spread(key, head_dim, length)
            query_inv = lax.rsqrt(
                mxu_fine(jnp.square(query.astype(jnp.float32)), lane_ones, NN) + 1.0
            )
            cosine = mxu(query, tall, NT) * query_inv * key_row_inv(tall)
            scores = scale_ref[g] * cosine + bias_ref[g] + mask
            expo = jnp.exp(scores - segment_max(scores, length))
            probs = expo / mxu_fine(expo, wide_ones, NN)
            attended = mxu(probs.astype(jnp.bfloat16), spread(value, head_dim, length), NN)
            att_ref[
                pl.ds(pl.multiple_of(w * length, length), length), g * lanes : (g + 1) * lanes
            ] = attended.astype(jnp.bfloat16)
            probs_ref[w, g] = probs
            cos_ref[w, g] = cosine
        return carry

    lax.fori_loop(0, count, forward, 0)

    proj = mxu(att_ref[...], w_proj_ref[...], NN)
    centre = proj - jnp.mean(proj, -1, keepdims=True)
    inv_std = lax.rsqrt(jnp.mean(centre * centre, -1, keepdims=True) + EPS_NORM)
    normed = centre * inv_std
    upstream = grad_ref[...].astype(jnp.float32)
    d_gain_ref[...] = jnp.sum(upstream * normed, 0, keepdims=True)
    scaled = upstream * gain_ref[...]
    d_proj = inv_std * (
        scaled
        - jnp.mean(scaled, -1, keepdims=True)
        - normed * jnp.mean(scaled * normed, -1, keepdims=True)
    )
    d_proj = d_proj.astype(jnp.bfloat16)
    d_wproj_ref[...] = mxu(att_ref[...], d_proj, TN)
    d_att_ref[...] = mxu(d_proj, w_proj_ref[...], NT).astype(jnp.bfloat16)
    d_bias_ref[...] = jnp.zeros_like(d_bias_ref)
    d_cos_ref[...] = jnp.zeros_like(d_cos_ref)

    def backward(w, carry):
        rows = pl.ds(pl.multiple_of(w * length, length), length)
        for g in range(groups):
            query, key, value = load(w, g, 0), load(w, g, 1), load(w, g, 2)
            d_att = d_att_ref[rows, g * lanes : (g + 1) * lanes]
            probs = probs_ref[w, g]
            cosine = cos_ref[w, g]
            tall = spread(key, head_dim, length)
            d_probs = mxu(d_att, spread(value, head_dim, length), NT)
            d_value = gather_heads(
                mxu(probs.astype(jnp.bfloat16), d_att, TN), head_dim, length
            )
            d_scores = probs * (d_probs - mxu_fine(d_probs * probs, wide_ones, NN))
            d_bias_ref[g] += d_scores
            d_cos_ref[g] += d_scores * cosine
            scaled_scores = d_scores * scale_ref[g]
            query32, key32 = query.astype(jnp.float32), key.astype(jnp.float32)
            query_sum = mxu_fine(jnp.square(query32), lane_ones, NN)
            query_wide = lax.rsqrt(query_sum + 1.0)
            query_inv = lax.rsqrt(mxu_fine(jnp.square(query32), lane_lane, NN) + 1.0)
            key_inv = lax.rsqrt(mxu_fine(jnp.square(key32), lane_lane, NN) + 1.0)
            d_unit_q = mxu_fine(scaled_scores * key_row_inv(tall), tall, NN)
            d_unit_k = gather_heads(
                mxu_fine(scaled_scores * query_wide, query, TN), head_dim, length
            )
            unit_q, unit_k = query32 * query_inv, key32 * key_inv
            d_query = query_inv * (d_unit_q - unit_q * mxu_fine(unit_q * d_unit_q, lane_lane, NN))
            d_key = key_inv * (d_unit_k - unit_k * mxu_fine(unit_k * d_unit_k, lane_lane, NN))
            for part, grad in enumerate((d_query, d_key, d_value)):
                d_qkv_ref[rows, part * depth + g * lanes : part * depth + (g + 1) * lanes] = (
                    grad.astype(jnp.bfloat16)
                )
        return carry

    lax.fori_loop(0, count, backward, 0)
    d_wqkv_ref[...] = mxu(flat_ref[...], d_qkv_ref[...], TN)
    d_flat_ref[...] = mxu(d_qkv_ref[...], w_qkv_ref[...], NT).astype(jnp.bfloat16)


def offset_onehot(window):
    places = np.arange(window * window)
    row_of, col_of = places // window, places % window
    offset = (row_of[:, None] - row_of[None, :] + window - 1) * (2 * window - 1) + (
        col_of[:, None] - col_of[None, :] + window - 1
    )
    return jnp.asarray(offset.reshape(-1), jnp.int32)


def three_parts(value):
    high = lax.reduce_precision(value, 8, 7)
    middle = lax.reduce_precision(value - high, 8, 7)
    return jnp.concatenate([high, middle, value - high - middle], 0).astype(jnp.bfloat16)


def local_grads(block, grad_block, row_base, col_base, height, width, window, params):
    w_qkv, w_proj, table_logits, logit_scale, gain = params
    images, rows, cols, depth = block.shape
    heads = logit_scale.shape[0]
    length = window * window
    groups = heads // GROUP
    wide = GROUP * length
    flat = to_windows(block, window).reshape(-1, depth)
    grad_flat = to_windows(grad_block, window).reshape(-1, depth)
    tokens = flat.shape[0]
    count = tokens // length
    scale = jnp.exp(jnp.minimum(logit_scale, SCALE_CAP))
    scale_rows = jnp.repeat(scale.reshape(groups, GROUP), length, 1).reshape(groups, 1, wide)
    sigma = jax.nn.sigmoid(table_logits)
    entries = table_logits.shape[1]
    hot = offset_onehot(window)[None, :] == jnp.arange(entries, dtype=jnp.int32)[:, None]
    hot = hot.astype(jnp.bfloat16)
    parts = jnp.dot(three_parts(sigma * BIAS_RANGE), hot, preferred_element_type=jnp.float32)
    rel_bias = jnp.sum(parts.reshape(3, heads, -1), 0).reshape(groups, GROUP, length, length)
    rel_bias = rel_bias.transpose(0, 2, 1, 3).reshape(groups, length, wide)
    f32, b16 = jnp.float32, jnp.bfloat16
    d_flat, d_wqkv, d_wproj, d_bias, d_cos, d_gain = pl.pallas_call(
        functools.partial(local_kernel, cols // window, height, width, window),
        out_shape=[
            jax.ShapeDtypeStruct((tokens, depth), b16),
            jax.ShapeDtypeStruct((depth, 3 * depth), f32),
            jax.ShapeDtypeStruct((depth, depth), f32),
            jax.ShapeDtypeStruct((groups, length, wide), f32),
            jax.ShapeDtypeStruct((groups, length, wide), f32),
            jax.ShapeDtypeStruct((1, depth), f32),
        ],
        in_specs=[VMEM] * 7,
        out_specs=[VMEM] * 6,
        scratch_shapes=[
            pltpu.VMEM((tokens, 3 * depth), b16),
            pltpu.VMEM((tokens, depth), b16),
            pltpu.VMEM((tokens, depth), b16),
            pltpu.VMEM((tokens, 3 * depth), b16),
            pltpu.VMEM((count, groups, length, wide), f32),
            pltpu.VMEM((count, groups, length, wide), f32),
        ],
        compiler_params=pltpu.CompilerParams(vmem_limit_bytes=48 * 2**20),
        cost_estimate=pl.CostEstimate(
            flops=4_000_000_000, bytes_accessed=8_000_000, transcendentals=400_000
        ),
        name="local_grads",
    )(flat, grad_flat, w_qkv, w_proj, rel_bias, scale_rows, gain.reshape(1, depth))
    heads_bias = d_bias.reshape(groups, length, GROUP, length).transpose(0, 2, 1, 3)
    heads_bias = heads_bias.reshape(heads, length * length)
    sums = lax.dot_general(three_parts(heads_bias), hot, NT, preferred_element_type=jnp.float32)
    d_table = jnp.sum(sums.reshape(3, heads, entries), 0) * (BIAS_RANGE * sigma * (1.0 - sigma))
    live = (logit_scale < SCALE_CAP).astype(jnp.float32)
    d_scale = jnp.sum(d_cos.reshape(groups, length, GROUP, length), (1, 3)).reshape(heads)
    d_scale = d_scale * scale * live
    d_block = from_windows(d_flat.reshape(images, count, length, depth), images, rows, cols, window)
    return (d_block, (d_wqkv, d_wproj, d_table, d_scale, d_gain.reshape(depth)))


def reduce_kernel(
    shape, wqkv_ref, wproj_ref, small_ref, qkv_out, proj_out, small_out,
    core_send, core_get, image_keep, image_send, image_get, near_send, near_get, own, whole, core_all,
    small_core, small_image, small_a, small_b, small_near,
    core_sems, image_sems, near_sems, all_sems, last_sems, tiny_sems,
):
    size_h, size_w = shape
    chips = size_h // 2
    peers = chips * size_w
    ha, wa, ba = lax.axis_index("ha"), lax.axis_index("wa"), lax.axis_index("ba")
    core = ha % 2
    me = wa * chips + ha // 2
    partner = (ha + 1 - 2 * core, wa, ba)
    image = (ha, wa, 1 - ba)

    def peer(step):
        other = lax.rem(me + step, peers)
        return other, (other % chips * 2 + core, other // chips, ba)

    barrier = pltpu.get_barrier_semaphore()
    pl.semaphore_signal(barrier, inc=1, device_id=partner, device_id_type=MESH)
    pl.semaphore_signal(barrier, inc=1, device_id=image, device_id_type=MESH)
    for step in range(1, peers):
        pl.semaphore_signal(barrier, inc=1, device_id=peer(step)[1], device_id_type=MESH)

    depth = wqkv_ref.shape[0]
    half = depth // 2
    q_half, p_half = wqkv_ref.shape[1] // 2, wproj_ref.shape[1] // 2
    f32, b16 = jnp.float32, jnp.bfloat16
    mine = pl.ds(pl.multiple_of(core * half, 16), half)
    theirs = pl.ds(pl.multiple_of((1 - core) * half, 16), half)
    core_send[:, : 2 * q_half] = wqkv_ref[theirs, :].astype(b16)
    core_send[:, 2 * q_half :] = wproj_ref[theirs, :].astype(b16)
    pl.semaphore_wait(barrier, peers + 1)

    def start(src, dst, sems, device):
        copy = pltpu.make_async_remote_copy(
            src_ref=src, dst_ref=dst, send_sem=sems.at[0], recv_sem=sems.at[1],
            device_id=device, device_id_type=MESH,
        )
        copy.start()
        return copy

    big = start(core_send, core_get, core_sems, partner)
    tiny = start(small_ref, small_core, tiny_sems.at[0], partner)
    tiny.wait()
    small_a[...] = small_ref[...] + small_core[...]
    tiny = start(small_a, small_image, tiny_sems.at[1], image)
    big.wait()

    def halves(first):
        q = wqkv_ref[mine, first * q_half : (first + 1) * q_half]
        p = wproj_ref[mine, first * p_half : (first + 1) * p_half]
        gq = core_get[:, first * q_half : (first + 1) * q_half]
        gp = core_get[:, 2 * q_half + first * p_half : 2 * q_half + (first + 1) * p_half]
        return q + gq.astype(f32), p + gp.astype(f32)

    low, high = halves(0), halves(1)
    for part, (a, b) in enumerate(zip(low, high)):
        place = slice(0, q_half) if part == 0 else slice(q_half, q_half + p_half)
        image_send[:, place] = jnp.where(ba == 0, b, a).astype(b16)
        image_keep[:, place] = jnp.where(ba == 0, a, b)
    big = start(image_send, image_get, image_sems, image)
    tiny.wait()
    small_b[...] = small_a[...] + small_image[...]
    tinies = []
    for step in range(1, peers):
        tinies.append(start(small_b, small_near.at[step - 1], tiny_sems.at[step + 1], peer(step)[1]))
    big.wait()
    total = image_keep[...] + image_get[...].astype(f32)
    r, c = near_send.shape[1:]
    split_c = total.shape[1] // c
    for j in range(peers):
        row, col = j // split_c * r, j % split_c * c
        near_send[j] = total[row : row + r, col : col + c].astype(b16)
    copies = []
    for step in range(1, peers):
        other, device = peer(step)
        copies.append(start(near_send.at[other], near_get.at[step - 1], near_sems.at[step - 1], device))
    for copy in tinies:
        copy.wait()
    small = small_b[...]
    for step in range(1, peers):
        small = small + small_near[step - 1]
    small_out[...] = small
    for copy in copies:
        copy.wait()
    total = near_send[me].astype(f32)
    for step in range(1, peers):
        total = total + near_get[step - 1].astype(f32)
    own[...] = total.astype(b16)
    whole[me] = own[...]
    copies = []
    for step in range(1, peers):
        _, device = peer(step)
        copies.append(start(own, whole.at[me], all_sems.at[step - 1], device))
    for copy in copies:
        copy.wait()
    last = start(whole, core_all, last_sems, partner)

    def put(source, first):
        for j in range(peers):
            row, col = j // split_c * r, j % split_c * c
            block = source[j].astype(f32)
            rows = pl.ds(pl.multiple_of(first * half + row, 8), r)
            q_part = max(0, min(c, q_half - col))
            if q_part > 0:
                qkv_out[rows, col : col + q_part] = block[:, :q_part]
            if q_part < c:
                begin = col + q_part - q_half
                proj_out[rows, begin : begin + c - q_part] = block[:, q_part:]

    put(whole, core)
    last.wait()
    put(core_all, 1 - core)


def reduce_all(d_wqkv, d_wproj, small):
    size_h, size_w = lax.axis_size("ha"), lax.axis_size("wa")
    peers = size_h // 2 * size_w
    depth = d_wqkv.shape[0]
    half = depth // 2
    cols = (d_wqkv.shape[1] + d_wproj.shape[1]) // 2
    split_c = 2
    r, c = half * split_c // peers, cols // split_c
    f32, b16 = jnp.float32, jnp.bfloat16
    tiny = small.shape
    return pl.pallas_call(
        functools.partial(reduce_kernel, (size_h, size_w)),
        out_shape=[
            jax.ShapeDtypeStruct((depth, d_wqkv.shape[1] // 2), f32),
            jax.ShapeDtypeStruct((depth, d_wproj.shape[1] // 2), f32),
            jax.ShapeDtypeStruct(tiny, f32),
        ],
        in_specs=[VMEM] * 3,
        out_specs=[VMEM] * 3,
        scratch_shapes=[
            pltpu.VMEM((half, 2 * cols), b16),
            pltpu.VMEM((half, 2 * cols), b16),
            pltpu.VMEM((half, cols), f32),
            pltpu.VMEM((half, cols), b16),
            pltpu.VMEM((half, cols), b16),
            pltpu.VMEM((peers, r, c), b16),
            pltpu.VMEM((peers - 1, r, c), b16),
            pltpu.VMEM((r, c), b16),
            pltpu.VMEM((peers, r, c), b16),
            pltpu.VMEM((peers, r, c), b16),
            pltpu.VMEM(tiny, f32),
            pltpu.VMEM(tiny, f32),
            pltpu.VMEM(tiny, f32),
            pltpu.VMEM(tiny, f32),
            pltpu.VMEM((peers - 1, *tiny), f32),
            pltpu.SemaphoreType.DMA((2,)),
            pltpu.SemaphoreType.DMA((2,)),
            pltpu.SemaphoreType.DMA((peers - 1, 2)),
            pltpu.SemaphoreType.DMA((peers - 1, 2)),
            pltpu.SemaphoreType.DMA((2,)),
            pltpu.SemaphoreType.DMA((peers + 1, 2)),
        ],
        compiler_params=pltpu.CompilerParams(
            collective_id=0, has_side_effects=True, vmem_limit_bytes=48 * 2**20
        ),
        name="reduce_all",
    )(d_wqkv, d_wproj, small)


def can_reduce(d_wqkv):
    peers = lax.axis_size("ha") // 2 * lax.axis_size("wa")
    pairs = lax.axis_size("ha") % 2 == 0 and lax.axis_size("ba") == 2
    return pairs and peers > 1 and d_wqkv.shape[0] % peers == 0 and d_wqkv.shape[0] // peers % 16 == 0


def pack_small(d_table, d_scale, d_gain):
    heads, entries = d_table.shape
    lanes = -(-entries // 128) * 128
    flat = jnp.concatenate([d_scale, d_gain])
    rows = -(-flat.shape[0] // lanes)
    flat = jnp.pad(flat, (0, rows * lanes - flat.shape[0])).reshape(rows, lanes)
    table = jnp.pad(d_table, ((0, 0), (0, lanes - entries)))
    full = jnp.concatenate([table, flat], 0)
    return jnp.pad(full, ((0, -full.shape[0] % 8), (0, 0)))


def unpack_small(full, heads, entries, depth):
    flat = full[heads:].reshape(-1)
    return full[:heads, :entries], flat[:heads], flat[heads : heads + depth]


def shift_in(tokens, cotangent, shift):
    stacked = jnp.stack([tokens, cotangent])
    below = from_behind(stacked[:, :, :shift], "ha", -1)
    tall = jnp.concatenate([stacked[:, :, shift:], below], 2)
    beside = from_behind(tall[:, :, :, :shift], "wa", -1)
    moved = jnp.concatenate([tall[:, :, :, shift:], beside], 3)
    return (moved[0], moved[1])


def shift_out(grads, shift):
    rows = grads.shape[1]
    cols = grads.shape[2]
    right = from_behind(grads[:, :, cols - shift :], "wa", 1)
    wide = jnp.concatenate([right, grads[:, :, : cols - shift]], 2)
    lower = from_behind(wide[:, rows - shift :], "ha", 1)
    return jnp.concatenate([lower, wide[:, : rows - shift]], 1)


def shards(tokens, cotangent, w_qkv, w_proj, table_logits, logit_scale, gain):
    rows = tokens.shape[1]
    cols = tokens.shape[2]
    shift = WIN // 2
    height = rows * lax.axis_size("ha")
    width = cols * lax.axis_size("wa")
    row_base = lax.axis_index("ha") * rows
    col_base = lax.axis_index("wa") * cols
    params = (w_qkv, w_proj, table_logits, logit_scale, gain)
    moved, moved_grad = shift_in(tokens, cotangent, shift)
    d_moved, parts = local_grads(moved, moved_grad, row_base, col_base, height, width, WIN, params)
    back = shift_out(d_moved, shift)
    d_tokens = (cotangent.astype(jnp.float32) + back.astype(jnp.float32)).astype(jnp.bfloat16)
    d_wqkv, d_wproj, d_table, d_scale, d_gain = parts
    if can_reduce(d_wqkv):
        small = pack_small(d_table, d_scale, d_gain)
        half_qkv, half_proj, small = reduce_all(d_wqkv, d_wproj, small)
        d_table, d_scale, d_gain = unpack_small(small, *d_table.shape, d_gain.shape[0])
    else:
        half_qkv, half_proj = (
            lax.psum_scatter(d_wqkv.astype(jnp.bfloat16), "ba", scatter_dimension=1, tiled=True).astype(
                jnp.float32
            ),
            lax.psum_scatter(
                d_wproj.astype(jnp.bfloat16), "ba", scatter_dimension=1, tiled=True
            ).astype(jnp.float32),
        )
        half_qkv, half_proj = lax.psum((half_qkv, half_proj), ("ha", "wa"))
        d_table, d_scale, d_gain = lax.psum((d_table, d_scale, d_gain), ("ha", "wa", "ba"))
    return (d_tokens, half_qkv, half_proj, d_table, d_scale, d_gain)


def solution(mesh):
    return jax.shard_map(
        shards,
        mesh=mesh,
        in_specs=(P("ba", "ha", "wa", None), P("ba", "ha", "wa", None), P(), P(), P(), P(), P()),
        out_specs=(P("ba", "ha", "wa", None), P(None, "ba"), P(None, "ba"), P(), P(), P()),
        check_vma=False,
    )
```

```python
import math

import functools

import jax
import jax.numpy as jnp
import numpy as np
from jax import lax
from jax.experimental import pallas as pl
from jax.experimental.pallas import tpu as pltpu
from jax.sharding import PartitionSpec as P

WIN = 8


EPS_NORM = 1e-05
MASK_FILL = -100.0
SCALE_CAP = math.log(100.0)
BIAS_RANGE = 16.0


def from_behind(block, axis, distance):
    devices = range(lax.axis_size(axis))
    route = [((i - distance) % len(devices), i) for i in devices]
    return lax.ppermute(block, axis, route)


def from_windows(tiles, images, height, width, window):
    depth = tiles.shape[-1]
    grid = tiles.reshape(images, height // window, width // window, window, window, depth)
    return grid.transpose(0, 1, 3, 2, 4, 5).reshape(images, height, width, depth)


def region_of(coords, extent, window):
    return (coords >= extent - window).astype(jnp.int32) + (coords >= extent - window // 2).astype(
        jnp.int32
    )

GROUP = 4
MESH = pl.DeviceIdType.MESH
VMEM = pl.BlockSpec(memory_space=pltpu.VMEM)
NN = (((1,), (0,)), ((), ()))
NT = (((1,), (1,)), ((), ()))
TN = (((0,), (0,)), ((), ()))


def mxu(left, right, dims):
    return lax.dot_general(left, right, dims, preferred_element_type=jnp.float32)


def split(value):
    high = value.astype(jnp.bfloat16)
    return high, (value - high.astype(jnp.float32)).astype(jnp.bfloat16)


def mxu_fine(left, right, dims):
    high, low = split(left)
    return mxu(high, right, dims) + mxu(low, right, dims)


def same_block(rows, cols, row_size, col_size):
    row = lax.broadcasted_iota(jnp.int32, (rows, cols), 0) // row_size
    col = lax.broadcasted_iota(jnp.int32, (rows, cols), 1) // col_size
    return (row == col).astype(jnp.bfloat16)


def spread(value, width, length):
    tall = jnp.concatenate([value] * GROUP, 0)
    return tall * same_block(tall.shape[0], tall.shape[1], length, width)


def gather_heads(value, width, length):
    lane = lax.broadcasted_iota(jnp.int32, (length, value.shape[1]), 1) // width
    total = jnp.where(lane == 0, value[:length], 0.0)
    for head in range(1, GROUP):
        total = jnp.where(lane == head, value[head * length : (head + 1) * length], total)
    return total


def segment_max(value, size):
    lane = lax.broadcasted_iota(jnp.int32, value.shape, 1) // size
    top = jnp.zeros_like(value)
    for head in range(value.shape[1] // size):
        here = jnp.max(jnp.where(lane == head, value, -jnp.inf), -1, keepdims=True)
        top = jnp.where(lane == head, here, top)
    return top


def local_kernel(
    grid_cols, height, width, window,
    flat_ref, grad_ref, w_qkv_ref, w_proj_ref, bias_ref, scale_ref, gain_ref,
    d_flat_ref, d_wqkv_ref, d_wproj_ref, d_bias_ref, d_cos_ref, d_gain_ref,
    qkv_ref, att_ref, d_att_ref, d_qkv_ref, probs_ref, cos_ref,
):
    tokens, depth = flat_ref.shape
    length = window * window
    count = tokens // length
    groups = bias_ref.shape[0]
    lanes = depth // groups
    head_dim = lanes // GROUP
    wide = GROUP * length
    row_base = lax.axis_index("ha") * (count // grid_cols * window)
    col_base = lax.axis_index("wa") * (grid_cols * window)

    qkv_ref[...] = mxu(flat_ref[...], w_qkv_ref[...], NN).astype(jnp.bfloat16)
    lane_ones = same_block(lanes, wide, head_dim, length)
    wide_ones = same_block(wide, wide, length, length)
    lane_lane = same_block(lanes, lanes, head_dim, head_dim)
    row_ones = jnp.ones((8, lanes), jnp.bfloat16)

    def labels(place, first_row, first_col):
        place = place % length
        row = first_row + place // window
        col = first_col + (place + window // 2) % window
        return region_of(row, height, window) * 3 + region_of(col, width, window)

    def load(w, g, part):
        return qkv_ref[
            pl.ds(pl.multiple_of(w * length, length), length),
            part * depth + g * lanes : part * depth + (g + 1) * lanes,
        ]

    def key_row_inv(tall):
        high, low = split(jnp.square(tall.astype(jnp.float32)))
        total = mxu(row_ones, high, NT) + mxu(row_ones, low, NT)
        return lax.rsqrt(total[:1] + 1.0)

    def forward(w, carry):
        first_row = row_base + w // grid_cols * window
        first_col = col_base + w % grid_cols * window
        shape = (length, wide)
        mine = labels(lax.broadcasted_iota(jnp.int32, shape, 0), first_row, first_col)
        other = labels(lax.broadcasted_iota(jnp.int32, shape, 1), first_row, first_col)
        mask = jnp.where(mine != other, MASK_FILL, 0.0)
        for g in range(groups):
            query, key, value = load(w, g, 0), load(w, g, 1), load(w, g, 2)
            tall = spread(key, head_dim, length)
            query_inv = lax.rsqrt(
                mxu_fine(jnp.square(query.astype(jnp.float32)), lane_ones, NN) + 1.0
            )
            cosine = mxu(query, tall, NT) * query_inv * key_row_inv(tall)
            scores = scale_ref[g] * cosine + bias_ref[g] + mask
            expo = jnp.exp(scores - segment_max(scores, length))
            probs = expo / mxu_fine(expo, wide_ones, NN)
            attended = mxu(probs.astype(jnp.bfloat16), spread(value, head_dim, length), NN)
            att_ref[
                pl.ds(pl.multiple_of(w * length, length), length), g * lanes : (g + 1) * lanes
            ] = attended.astype(jnp.bfloat16)
            probs_ref[w, g] = probs
            cos_ref[w, g] = cosine
        return carry

    lax.fori_loop(0, count, forward, 0)

    proj = mxu(att_ref[...], w_proj_ref[...], NN)
    centre = proj - jnp.mean(proj, -1, keepdims=True)
    inv_std = lax.rsqrt(jnp.mean(centre * centre, -1, keepdims=True) + EPS_NORM)
    normed = centre * inv_std
    upstream = grad_ref[...].astype(jnp.float32)
    d_gain_ref[...] = jnp.sum(upstream * normed, 0, keepdims=True)
    scaled = upstream * gain_ref[...]
    d_proj = inv_std * (
        scaled
        - jnp.mean(scaled, -1, keepdims=True)
        - normed * jnp.mean(scaled * normed, -1, keepdims=True)
    )
    d_proj = d_proj.astype(jnp.bfloat16)
    d_wproj_ref[...] = mxu(att_ref[...], d_proj, TN)
    d_att_ref[...] = mxu(d_proj, w_proj_ref[...], NT).astype(jnp.bfloat16)
    d_bias_ref[...] = jnp.zeros_like(d_bias_ref)
    d_cos_ref[...] = jnp.zeros_like(d_cos_ref)

    def backward(w, carry):
        rows = pl.ds(pl.multiple_of(w * length, length), length)
        for g in range(groups):
            query, key, value = load(w, g, 0), load(w, g, 1), load(w, g, 2)
            d_att = d_att_ref[rows, g * lanes : (g + 1) * lanes]
            probs = probs_ref[w, g]
            cosine = cos_ref[w, g]
            tall = spread(key, head_dim, length)
            d_probs = mxu(d_att, spread(value, head_dim, length), NT)
            d_value = gather_heads(
                mxu(probs.astype(jnp.bfloat16), d_att, TN), head_dim, length
            )
            d_scores = probs * (d_probs - mxu_fine(d_probs * probs, wide_ones, NN))
            d_bias_ref[g] += d_scores
            d_cos_ref[g] += d_scores * cosine
            scaled_scores = d_scores * scale_ref[g]
            query32, key32 = query.astype(jnp.float32), key.astype(jnp.float32)
            query_sum = mxu_fine(jnp.square(query32), lane_ones, NN)
            query_wide = lax.rsqrt(query_sum + 1.0)
            query_inv = lax.rsqrt(mxu_fine(jnp.square(query32), lane_lane, NN) + 1.0)
            key_inv = lax.rsqrt(mxu_fine(jnp.square(key32), lane_lane, NN) + 1.0)
            d_unit_q = mxu_fine(scaled_scores * key_row_inv(tall), tall, NN)
            d_unit_k = gather_heads(
                mxu_fine(scaled_scores * query_wide, query, TN), head_dim, length
            )
            unit_q, unit_k = query32 * query_inv, key32 * key_inv
            d_query = query_inv * (d_unit_q - unit_q * mxu_fine(unit_q * d_unit_q, lane_lane, NN))
            d_key = key_inv * (d_unit_k - unit_k * mxu_fine(unit_k * d_unit_k, lane_lane, NN))
            for part, grad in enumerate((d_query, d_key, d_value)):
                d_qkv_ref[rows, part * depth + g * lanes : part * depth + (g + 1) * lanes] = (
                    grad.astype(jnp.bfloat16)
                )
        return carry

    lax.fori_loop(0, count, backward, 0)
    d_wqkv_ref[...] = mxu(flat_ref[...], d_qkv_ref[...], TN)
    d_flat_ref[...] = mxu(d_qkv_ref[...], w_qkv_ref[...], NT).astype(jnp.bfloat16)


def offset_onehot(window):
    places = np.arange(window * window)
    row_of, col_of = places // window, (places + window // 2) % window
    offset = (row_of[:, None] - row_of[None, :] + window - 1) * (2 * window - 1) + (
        col_of[:, None] - col_of[None, :] + window - 1
    )
    return jnp.asarray(offset.reshape(-1), jnp.int32)


def three_parts(value):
    high = lax.reduce_precision(value, 8, 7)
    middle = lax.reduce_precision(value - high, 8, 7)
    return jnp.concatenate([high, middle, value - high - middle], 0).astype(jnp.bfloat16)


def local_grads(flat, grad_flat, cols, height, width, window, params):
    w_qkv, w_proj, table_logits, logit_scale, gain = params
    depth = flat.shape[1]
    heads = logit_scale.shape[0]
    length = window * window
    groups = heads // GROUP
    wide = GROUP * length
    tokens = flat.shape[0]
    count = tokens // length
    scale = jnp.exp(jnp.minimum(logit_scale, SCALE_CAP))
    scale_rows = jnp.repeat(scale.reshape(groups, GROUP), length, 1).reshape(groups, 1, wide)
    sigma = jax.nn.sigmoid(table_logits)
    entries = table_logits.shape[1]
    hot = offset_onehot(window)[None, :] == jnp.arange(entries, dtype=jnp.int32)[:, None]
    hot = hot.astype(jnp.bfloat16)
    parts = jnp.dot(three_parts(sigma * BIAS_RANGE), hot, preferred_element_type=jnp.float32)
    rel_bias = jnp.sum(parts.reshape(3, heads, -1), 0).reshape(groups, GROUP, length, length)
    rel_bias = rel_bias.transpose(0, 2, 1, 3).reshape(groups, length, wide)
    f32, b16 = jnp.float32, jnp.bfloat16
    d_flat, d_wqkv, d_wproj, d_bias, d_cos, d_gain = pl.pallas_call(
        functools.partial(local_kernel, cols // window, height, width, window),
        out_shape=[
            jax.ShapeDtypeStruct((tokens, depth), b16),
            jax.ShapeDtypeStruct((depth, 3 * depth), f32),
            jax.ShapeDtypeStruct((depth, depth), f32),
            jax.ShapeDtypeStruct((groups, length, wide), f32),
            jax.ShapeDtypeStruct((groups, length, wide), f32),
            jax.ShapeDtypeStruct((1, depth), f32),
        ],
        in_specs=[VMEM] * 7,
        out_specs=[VMEM] * 6,
        scratch_shapes=[
            pltpu.VMEM((tokens, 3 * depth), b16),
            pltpu.VMEM((tokens, depth), b16),
            pltpu.VMEM((tokens, depth), b16),
            pltpu.VMEM((tokens, 3 * depth), b16),
            pltpu.VMEM((count, groups, length, wide), f32),
            pltpu.VMEM((count, groups, length, wide), f32),
        ],
        compiler_params=pltpu.CompilerParams(vmem_limit_bytes=48 * 2**20),
        cost_estimate=pl.CostEstimate(
            flops=4_000_000_000, bytes_accessed=8_000_000, transcendentals=400_000
        ),
        name="local_grads",
    )(flat, grad_flat, w_qkv, w_proj, rel_bias, scale_rows, gain.reshape(1, depth))
    heads_bias = d_bias.reshape(groups, length, GROUP, length).transpose(0, 2, 1, 3)
    heads_bias = heads_bias.reshape(heads, length * length)
    sums = lax.dot_general(three_parts(heads_bias), hot, NT, preferred_element_type=jnp.float32)
    d_table = jnp.sum(sums.reshape(3, heads, entries), 0) * (BIAS_RANGE * sigma * (1.0 - sigma))
    live = (logit_scale < SCALE_CAP).astype(jnp.float32)
    d_scale = jnp.sum(d_cos.reshape(groups, length, GROUP, length), (1, 3)).reshape(heads)
    d_scale = d_scale * scale * live
    return (d_flat, (d_wqkv, d_wproj, d_table, d_scale, d_gain.reshape(depth)))


def shift_in_kernel(
    size_h, size_w, window, tokens_ref, cot_ref, flat_ref, grad_ref,
    side_send, row_get, side_get, corner_get, sems,
):
    ha, wa, ba = lax.axis_index("ha"), lax.axis_index("wa"), lax.axis_index("ba")
    up, left = lax.rem(ha + size_h - 1, size_h), lax.rem(wa + size_w - 1, size_w)
    down, right = lax.rem(ha + 1, size_h), lax.rem(wa + 1, size_w)
    barrier = pltpu.get_barrier_semaphore()
    for device in ((down, wa, ba), (ha, right, ba), (down, right, ba)):
        pl.semaphore_signal(barrier, inc=1, device_id=device, device_id_type=MESH)
    rows, cols, depth = tokens_ref.shape
    shift = window // 2
    tiles = cols // window
    f32 = jnp.float32
    for n, ref in enumerate((tokens_ref, cot_ref)):
        side = ref[:, :window, :].astype(f32).reshape(rows * window, depth)
        side_send[n] = side.astype(jnp.bfloat16)
    pl.semaphore_wait(barrier, 3)
    copies = []
    for n, ref in enumerate((tokens_ref, cot_ref)):
        edge = shift * window
        plan = (
            (ref.at[pl.ds(0, shift)], row_get.at[n], (up, wa, ba)),
            (side_send.at[n], side_get.at[n], (ha, left, ba)),
            (side_send.at[n, pl.ds(0, edge)], corner_get.at[n], (up, left, ba)),
        )
        for k, (src, dst, device) in enumerate(plan):
            copy = pltpu.make_async_remote_copy(
                src_ref=src, dst_ref=dst, send_sem=sems.at[n, k, 0], recv_sem=sems.at[n, k, 1],
                device_id=device, device_id_type=MESH,
            )
            copy.start()
            copies.append(copy)
    for copy in copies:
        copy.wait()
    later = lax.broadcasted_iota(jnp.int32, (window, window, depth), 1) >= shift
    for n, (ref, out) in enumerate(((tokens_ref, flat_ref), (cot_ref, grad_ref))):
        tall = jnp.concatenate([ref[shift:].astype(f32), row_get[n].astype(f32)], 0)
        tall = tall.reshape(rows, tiles, window, depth)
        side = jnp.concatenate(
            [side_get[n, shift * window :].astype(f32), corner_get[n].astype(f32)], 0
        ).reshape(rows, window, depth)
        for down_tile in range(rows // window):
            span = slice(down_tile * window, (down_tile + 1) * window)
            for tile in range(tiles):
                beside = tall[span, tile + 1] if tile + 1 < tiles else side[span]
                value = jnp.where(later, tall[span, tile], beside)
                place = (down_tile * tiles + tile) * window * window
                out[place : place + window * window, :] = value.reshape(
                    window * window, depth
                ).astype(jnp.bfloat16)


def shift_in(tokens, cotangent, window):
    _, rows, cols, depth = tokens.shape
    b16 = jnp.bfloat16
    shift = window // 2
    flat = jax.ShapeDtypeStruct((rows * cols, depth), b16)
    return pl.pallas_call(
        functools.partial(shift_in_kernel, lax.axis_size("ha"), lax.axis_size("wa"), window),
        out_shape=[flat, flat],
        in_specs=[VMEM] * 2,
        out_specs=[VMEM] * 2,
        scratch_shapes=[
            pltpu.VMEM((2, rows * window, depth), b16),
            pltpu.VMEM((2, shift, cols, depth), b16),
            pltpu.VMEM((2, rows * window, depth), b16),
            pltpu.VMEM((2, shift * window, depth), b16),
            pltpu.SemaphoreType.DMA((2, 3, 2)),
        ],
        compiler_params=pltpu.CompilerParams(
            collective_id=1, has_side_effects=True, vmem_limit_bytes=32 * 2**20
        ),
        name="shift_in",
    )(tokens.reshape(rows, cols, depth), cotangent.reshape(rows, cols, depth))


CHUNKS = 3


def reduce_kernel(
    shape, window, wqkv_ref, wproj_ref, small_ref, d_flat_ref, cot_ref,
    qkv_out, proj_out, small_out, tokens_out,
    core_send, core_get, image_keep, image_send, image_get, near_send, near_get, own, whole, core_all,
    small_core, small_image, small_a, small_b, small_near, side_get, row_get, corner_get,
    core_sems, image_sems, near_sems, all_sems, last_sems, tiny_sems, halo_sems,
):
    size_h, size_w = shape
    chips = size_h // 2
    peers = chips * size_w
    ha, wa, ba = lax.axis_index("ha"), lax.axis_index("wa"), lax.axis_index("ba")
    core = ha % 2
    me = wa * chips + ha // 2
    partner = (ha + 1 - 2 * core, wa, ba)
    image = (ha, wa, 1 - ba)
    up, left = lax.rem(ha + size_h - 1, size_h), lax.rem(wa + size_w - 1, size_w)
    down, right = lax.rem(ha + 1, size_h), lax.rem(wa + 1, size_w)

    def peer(step):
        other = lax.rem(me + step, peers)
        return other, (other % chips * 2 + core, other // chips, ba)

    barrier = pltpu.get_barrier_semaphore()
    greeted = [partner, image, (up, wa, ba), (ha, left, ba), (up, left, ba)]
    greeted += [peer(step)[1] for step in range(1, peers)]
    for device in greeted:
        pl.semaphore_signal(barrier, inc=1, device_id=device, device_id_type=MESH)

    depth = wqkv_ref.shape[0]
    half = depth // 2
    q_half, p_half = wqkv_ref.shape[1] // 2, wproj_ref.shape[1] // 2
    span = image_keep.shape[2]
    f32, b16 = jnp.float32, jnp.bfloat16
    mine = pl.ds(pl.multiple_of(core * half, 16), half)
    theirs = pl.ds(pl.multiple_of((1 - core) * half, 16), half)

    def piece(rows, side, k):
        low, high = k * span, (k + 1) * span
        parts = []
        if low < q_half:
            parts.append(wqkv_ref[rows, side * q_half + low : side * q_half + min(high, q_half)])
        if high > q_half:
            begin = side * p_half + max(low, q_half) - q_half
            parts.append(wproj_ref[rows, begin : side * p_half + high - q_half])
        return jnp.concatenate(parts, 1) if len(parts) > 1 else parts[0]

    for k in range(CHUNKS):
        for side in range(2):
            core_send[k, :, side * span : (side + 1) * span] = piece(theirs, side, k).astype(b16)
    pl.semaphore_wait(barrier, len(greeted))

    def start(src, dst, sems, device):
        copy = pltpu.make_async_remote_copy(
            src_ref=src, dst_ref=dst, send_sem=sems.at[0], recv_sem=sems.at[1],
            device_id=device, device_id_type=MESH,
        )
        copy.start()
        return copy

    bigs = [start(core_send.at[0], core_get.at[0], core_sems.at[0], partner)]
    tiny = start(small_ref, small_core, tiny_sems.at[0], partner)
    for k in range(1, CHUNKS):
        bigs.append(start(core_send.at[k], core_get.at[k], core_sems.at[k], partner))

    rows_here, cols_here = cot_ref.shape[:2]
    shift = window // 2
    length = window * window
    edge = shift * window
    tiles, bands = cols_here // window, rows_here // window
    halos = []
    for band in range(bands):
        size = length if band < bands - 1 else length - edge
        place = (band * tiles + tiles - 1) * length
        halos.append(
            start(
                d_flat_ref.at[pl.ds(place, size)], side_get.at[pl.ds(band * length, size)],
                halo_sems.at[len(halos)], (ha, right, ba),
            )
        )
    for tile in range(tiles):
        place = ((bands - 1) * tiles + tile) * length + length - edge
        halos.append(
            start(
                d_flat_ref.at[pl.ds(place, edge)], row_get.at[tile],
                halo_sems.at[len(halos)], (down, wa, ba),
            )
        )
    place = bands * tiles * length - edge
    halos.append(
        start(
            d_flat_ref.at[pl.ds(place, edge)], corner_get, halo_sems.at[len(halos)],
            (down, right, ba),
        )
    )

    def to_image(k):
        low = piece(mine, 0, k) + core_get[k, :, :span].astype(f32)
        high = piece(mine, 1, k) + core_get[k, :, span:].astype(f32)
        image_send[k] = jnp.where(ba == 0, high, low).astype(b16)
        image_keep[k] = jnp.where(ba == 0, low, high)
        return start(image_send.at[k], image_get.at[k], image_sems.at[k], image)

    images = []
    for k in range(CHUNKS):
        bigs[k].wait()
        images.append(to_image(k))
        if k == 0:
            tiny.wait()
            small_a[...] = small_ref[...] + small_core[...]
            tiny = start(small_a, small_image, tiny_sems.at[1], image)

    r, c = near_send.shape[2:]
    split_c = span // c

    def place_of(j):
        return j // split_c * r, j % split_c * c

    nears, tinies = [], []
    for k in range(CHUNKS):
        images[k].wait()
        total = image_keep[k] + image_get[k].astype(f32)
        for j in range(peers):
            row, col = place_of(j)
            near_send[k, j] = total[row : row + r, col : col + c].astype(b16)
        copies = []
        for step in range(1, peers):
            other, device = peer(step)
            copies.append(
                start(
                    near_send.at[k, other], near_get.at[k, step - 1], near_sems.at[k, step - 1], device
                )
            )
        nears.append(copies)
        if k == 0:
            tiny.wait()
            small_b[...] = small_a[...] + small_image[...]
            for step in range(1, peers):
                tinies.append(
                    start(small_b, small_near.at[step - 1], tiny_sems.at[step + 1], peer(step)[1])
                )

    alls = []
    for k in range(CHUNKS):
        for copy in nears[k]:
            copy.wait()
        total = near_send[k, me].astype(f32)
        for step in range(1, peers):
            total = total + near_get[k, step - 1].astype(f32)
        own[k] = total.astype(b16)
        whole[k, me] = own[k]
        alls.append(
            [
                start(own.at[k], whole.at[k, me], all_sems.at[k, step - 1], peer(step)[1])
                for step in range(1, peers)
            ]
        )

    for copy in tinies:
        copy.wait()
    small = small_b[...]
    for step in range(1, peers):
        small = small + small_near[step - 1]
    small_out[...] = small

    for copy in halos:
        copy.wait()
    depth_here = cot_ref.shape[2]
    later = lax.broadcasted_iota(jnp.int32, (1, window, depth_here), 1) >= shift

    def moved_tile(tile, first, count):
        parts = []
        for band in range(bands):
            begin, end = max(first, band * window), min(first + count, (band + 1) * window)
            if begin < end:
                source, base = d_flat_ref, (band * tiles + tile) * length
                if tile < 0:
                    source, base = side_get, band * length
                low = base + (begin - band * window) * window
                parts.append(source[low : low + (end - begin) * window, :])
        value = [part.astype(f32).reshape(-1, window, depth_here) for part in parts]
        return jnp.concatenate(value, 0)

    def above_tile(tile):
        value = corner_get[...] if tile < 0 else row_get[tile]
        return value.astype(f32).reshape(shift, window, depth_here)

    body = rows_here - shift
    for first in range(0, body, shift):
        grads = [moved_tile(tile, first, shift) for tile in range(-1, tiles)]
        wide = [jnp.where(later, grads[n + 1], grads[n]) for n in range(tiles)]
        wide = jnp.concatenate([x[:, None] for x in wide], 1).reshape(shift, cols_here, depth_here)
        there = slice(first + shift, first + 2 * shift)
        tokens_out[there] = (cot_ref[there].astype(f32) + wide).astype(b16)
    grads = [above_tile(tile) for tile in range(-1, tiles)]
    wide = [jnp.where(later, grads[n + 1], grads[n]) for n in range(tiles)]
    wide = jnp.concatenate([x[:, None] for x in wide], 1).reshape(shift, cols_here, depth_here)
    tokens_out[:shift] = (cot_ref[:shift].astype(f32) + wide).astype(b16)

    def put(source, k, first):
        for j in range(peers):
            row, col = place_of(j)
            col = col + k * span
            block = source[k, j].astype(f32)
            rows = pl.ds(pl.multiple_of(first * half + row, 8), r)
            q_part = max(0, min(c, q_half - col))
            if q_part > 0:
                qkv_out[rows, col : col + q_part] = block[:, :q_part]
            if q_part < c:
                begin = col + q_part - q_half
                proj_out[rows, begin : begin + c - q_part] = block[:, q_part:]

    lasts = []
    for k in range(CHUNKS):
        for copy in alls[k]:
            copy.wait()
        lasts.append(start(whole.at[k], core_all.at[k], last_sems.at[k], partner))
        put(whole, k, core)
    for k in range(CHUNKS):
        lasts[k].wait()
        put(core_all, k, 1 - core)


def reduce_all(d_wqkv, d_wproj, small, d_flat, cotangent, window):
    size_h, size_w = lax.axis_size("ha"), lax.axis_size("wa")
    peers = size_h // 2 * size_w
    depth = d_wqkv.shape[0]
    half = depth // 2
    cols = (d_wqkv.shape[1] + d_wproj.shape[1]) // 2 // CHUNKS
    split_c = 2
    r, c = half * split_c // peers, cols // split_c
    f32, b16 = jnp.float32, jnp.bfloat16
    tiny = small.shape
    _, rows_here, cols_here, channels = cotangent.shape
    tiles, bands = cols_here // window, rows_here // window
    length = window * window
    edge = length // 2
    quick, near = pltpu.SemaphoreType.DMA((CHUNKS, 2)), pltpu.SemaphoreType.DMA((CHUNKS, peers - 1, 2))
    *sums, d_tokens = pl.pallas_call(
        functools.partial(reduce_kernel, (size_h, size_w), window),
        out_shape=[
            jax.ShapeDtypeStruct((depth, d_wqkv.shape[1] // 2), f32),
            jax.ShapeDtypeStruct((depth, d_wproj.shape[1] // 2), f32),
            jax.ShapeDtypeStruct(tiny, f32),
            jax.ShapeDtypeStruct((rows_here, cols_here, channels), b16),
        ],
        in_specs=[VMEM] * 5,
        out_specs=[VMEM] * 4,
        scratch_shapes=[
            pltpu.VMEM((CHUNKS, half, 2 * cols), b16),
            pltpu.VMEM((CHUNKS, half, 2 * cols), b16),
            pltpu.VMEM((CHUNKS, half, cols), f32),
            pltpu.VMEM((CHUNKS, half, cols), b16),
            pltpu.VMEM((CHUNKS, half, cols), b16),
            pltpu.VMEM((CHUNKS, peers, r, c), b16),
            pltpu.VMEM((CHUNKS, peers - 1, r, c), b16),
            pltpu.VMEM((CHUNKS, r, c), b16),
            pltpu.VMEM((CHUNKS, peers, r, c), b16),
            pltpu.VMEM((CHUNKS, peers, r, c), b16),
            pltpu.VMEM(tiny, f32),
            pltpu.VMEM(tiny, f32),
            pltpu.VMEM(tiny, f32),
            pltpu.VMEM(tiny, f32),
            pltpu.VMEM((peers - 1, *tiny), f32),
            pltpu.VMEM((bands * length, channels), b16),
            pltpu.VMEM((tiles, edge, channels), b16),
            pltpu.VMEM((edge, channels), b16),
            quick,
            quick,
            near,
            near,
            quick,
            pltpu.SemaphoreType.DMA((peers + 1, 2)),
            pltpu.SemaphoreType.DMA((bands + tiles + 1, 2)),
        ],
        compiler_params=pltpu.CompilerParams(
            collective_id=0, has_side_effects=True, vmem_limit_bytes=48 * 2**20
        ),
        name="reduce_all",
    )(d_wqkv, d_wproj, small, d_flat, cotangent.reshape(rows_here, cols_here, channels))
    return (*sums, d_tokens.reshape(cotangent.shape))


def can_reduce(d_wqkv):
    peers = lax.axis_size("ha") // 2 * lax.axis_size("wa")
    pairs = lax.axis_size("ha") % 2 == 0 and lax.axis_size("ba") == 2
    return pairs and peers > 1 and d_wqkv.shape[0] % peers == 0 and d_wqkv.shape[0] // peers % 16 == 0


def pack_small(d_table, d_scale, d_gain):
    heads, entries = d_table.shape
    lanes = -(-entries // 128) * 128
    flat = jnp.concatenate([d_scale, d_gain])
    rows = -(-flat.shape[0] // lanes)
    flat = jnp.pad(flat, (0, rows * lanes - flat.shape[0])).reshape(rows, lanes)
    table = jnp.pad(d_table, ((0, 0), (0, lanes - entries)))
    full = jnp.concatenate([table, flat], 0)
    return jnp.pad(full, ((0, -full.shape[0] % 8), (0, 0)))


def unpack_small(full, heads, entries, depth):
    flat = full[heads:].reshape(-1)
    return full[:heads, :entries], flat[:heads], flat[heads : heads + depth]


def shift_out(grads, shift):
    rows = grads.shape[1]
    cols = grads.shape[2]
    right = from_behind(grads[:, :, cols - shift :], "wa", 1)
    wide = jnp.concatenate([right, grads[:, :, : cols - shift]], 2)
    lower = from_behind(wide[:, rows - shift :], "ha", 1)
    return jnp.concatenate([lower, wide[:, : rows - shift]], 1)


def shards(tokens, cotangent, w_qkv, w_proj, table_logits, logit_scale, gain):
    rows = tokens.shape[1]
    cols = tokens.shape[2]
    shift = WIN // 2
    height = rows * lax.axis_size("ha")
    width = cols * lax.axis_size("wa")
    params = (w_qkv, w_proj, table_logits, logit_scale, gain)
    flat, grad_flat = shift_in(tokens, cotangent, WIN)
    d_flat, parts = local_grads(flat, grad_flat, cols, height, width, WIN, params)
    d_wqkv, d_wproj, d_table, d_scale, d_gain = parts
    if can_reduce(d_wqkv):
        small = pack_small(d_table, d_scale, d_gain)
        half_qkv, half_proj, small, d_tokens = reduce_all(
            d_wqkv, d_wproj, small, d_flat, cotangent, WIN
        )
        d_table, d_scale, d_gain = unpack_small(small, *d_table.shape, d_gain.shape[0])
    else:
        turned = jnp.roll(d_flat.reshape(-1, WIN, d_flat.shape[1]), -shift, 1)
        turned = turned.reshape(-1, WIN * WIN, d_flat.shape[1])
        back = shift_out(from_windows(turned, tokens.shape[0], rows, cols, WIN), shift)
        d_tokens = (cotangent.astype(jnp.float32) + back.astype(jnp.float32)).astype(jnp.bfloat16)
        half_qkv, half_proj = (
            lax.psum_scatter(d_wqkv.astype(jnp.bfloat16), "ba", scatter_dimension=1, tiled=True).astype(
                jnp.float32
            ),
            lax.psum_scatter(
                d_wproj.astype(jnp.bfloat16), "ba", scatter_dimension=1, tiled=True
            ).astype(jnp.float32),
        )
        half_qkv, half_proj = lax.psum((half_qkv, half_proj), ("ha", "wa"))
        d_table, d_scale, d_gain = lax.psum((d_table, d_scale, d_gain), ("ha", "wa", "ba"))
    return (d_tokens, half_qkv, half_proj, d_table, d_scale, d_gain)


def solution(mesh):
    return jax.shard_map(
        shards,
        mesh=mesh,
        in_specs=(P("ba", "ha", "wa", None), P("ba", "ha", "wa", None), P(), P(), P(), P(), P()),
        out_specs=(P("ba", "ha", "wa", None), P(None, "ba"), P(None, "ba"), P(), P(), P()),
        check_vma=False,
    )
```

```python
import math

import functools

import jax
import jax.numpy as jnp
import numpy as np
from jax import lax
from jax.experimental import pallas as pl
from jax.experimental.pallas import tpu as pltpu
from jax.sharding import PartitionSpec as P

WIN = 8


EPS_NORM = 1e-05
MASK_FILL = -100.0
SCALE_CAP = math.log(100.0)
BIAS_RANGE = 16.0


def from_behind(block, axis, distance):
    devices = range(lax.axis_size(axis))
    route = [((i - distance) % len(devices), i) for i in devices]
    return lax.ppermute(block, axis, route)


def to_windows(block, window):
    images, height, width, depth = block.shape
    tiles = block.reshape(images, height // window, window, width // window, window, depth)
    tiles = tiles.transpose(0, 1, 3, 2, 4, 5)
    return tiles.reshape(images, height // window * (width // window), window * window, depth)


def from_windows(tiles, images, height, width, window):
    depth = tiles.shape[-1]
    grid = tiles.reshape(images, height // window, width // window, window, window, depth)
    return grid.transpose(0, 1, 3, 2, 4, 5).reshape(images, height, width, depth)


def region_of(coords, extent, window):
    return (coords >= extent - window).astype(jnp.int32) + (coords >= extent - window // 2).astype(
        jnp.int32
    )

GROUP = 4
MESH = pl.DeviceIdType.MESH
VMEM = pl.BlockSpec(memory_space=pltpu.VMEM)
NN = (((1,), (0,)), ((), ()))
NT = (((1,), (1,)), ((), ()))
TN = (((0,), (0,)), ((), ()))


def mxu(left, right, dims):
    return lax.dot_general(left, right, dims, preferred_element_type=jnp.float32)


def split(value):
    high = value.astype(jnp.bfloat16)
    return high, (value - high.astype(jnp.float32)).astype(jnp.bfloat16)


def mxu_fine(left, right, dims):
    high, low = split(left)
    return mxu(high, right, dims) + mxu(low, right, dims)


def same_block(rows, cols, row_size, col_size):
    row = lax.broadcasted_iota(jnp.int32, (rows, cols), 0) // row_size
    col = lax.broadcasted_iota(jnp.int32, (rows, cols), 1) // col_size
    return (row == col).astype(jnp.bfloat16)


def spread(value, width, length):
    tall = jnp.concatenate([value] * GROUP, 0)
    return tall * same_block(tall.shape[0], tall.shape[1], length, width)


def gather_heads(value, width, length):
    lane = lax.broadcasted_iota(jnp.int32, (length, value.shape[1]), 1) // width
    total = jnp.where(lane == 0, value[:length], 0.0)
    for head in range(1, GROUP):
        total = jnp.where(lane == head, value[head * length : (head + 1) * length], total)
    return total


def segment_max(value, size):
    lane = lax.broadcasted_iota(jnp.int32, value.shape, 1) // size
    top = jnp.zeros_like(value)
    for head in range(value.shape[1] // size):
        here = jnp.max(jnp.where(lane == head, value, -jnp.inf), -1, keepdims=True)
        top = jnp.where(lane == head, here, top)
    return top


def local_kernel(
    grid_cols, height, width, window,
    flat_ref, grad_ref, w_qkv_ref, w_proj_ref, bias_ref, scale_ref, gain_ref,
    d_flat_ref, d_wqkv_ref, d_wproj_ref, d_bias_ref, d_cos_ref, d_gain_ref,
    qkv_ref, att_ref, d_att_ref, d_qkv_ref, probs_ref, cos_ref,
):
    tokens, depth = flat_ref.shape
    length = window * window
    count = tokens // length
    groups = bias_ref.shape[0]
    lanes = depth // groups
    head_dim = lanes // GROUP
    wide = GROUP * length
    row_base = lax.axis_index("ha") * (count // grid_cols * window)
    col_base = lax.axis_index("wa") * (grid_cols * window)

    qkv_ref[...] = mxu(flat_ref[...], w_qkv_ref[...], NN).astype(jnp.bfloat16)
    lane_ones = same_block(lanes, wide, head_dim, length)
    wide_ones = same_block(wide, wide, length, length)
    lane_lane = same_block(lanes, lanes, head_dim, head_dim)
    row_ones = jnp.ones((8, lanes), jnp.bfloat16)

    def labels(place, first_row, first_col):
        place = place % length
        row = first_row + place // window
        col = first_col + place % window
        return region_of(row, height, window) * 3 + region_of(col, width, window)

    def load(w, g, part):
        return qkv_ref[
            pl.ds(pl.multiple_of(w * length, length), length),
            part * depth + g * lanes : part * depth + (g + 1) * lanes,
        ]

    def key_row_inv(tall):
        high, low = split(jnp.square(tall.astype(jnp.float32)))
        total = mxu(row_ones, high, NT) + mxu(row_ones, low, NT)
        return lax.rsqrt(total[:1] + 1.0)

    def forward(w, carry):
        first_row = row_base + w // grid_cols * window
        first_col = col_base + w % grid_cols * window
        shape = (length, wide)
        mine = labels(lax.broadcasted_iota(jnp.int32, shape, 0), first_row, first_col)
        other = labels(lax.broadcasted_iota(jnp.int32, shape, 1), first_row, first_col)
        mask = jnp.where(mine != other, MASK_FILL, 0.0)
        for g in range(groups):
            query, key, value = load(w, g, 0), load(w, g, 1), load(w, g, 2)
            tall = spread(key, head_dim, length)
            query_inv = lax.rsqrt(
                mxu_fine(jnp.square(query.astype(jnp.float32)), lane_ones, NN) + 1.0
            )
            cosine = mxu(query, tall, NT) * query_inv * key_row_inv(tall)
            scores = scale_ref[g] * cosine + bias_ref[g] + mask
            expo = jnp.exp(scores - segment_max(scores, length))
            probs = expo / mxu_fine(expo, wide_ones, NN)
            attended = mxu(probs.astype(jnp.bfloat16), spread(value, head_dim, length), NN)
            att_ref[
                pl.ds(pl.multiple_of(w * length, length), length), g * lanes : (g + 1) * lanes
            ] = attended.astype(jnp.bfloat16)
            probs_ref[w, g] = probs
            cos_ref[w, g] = cosine
        return carry

    lax.fori_loop(0, count, forward, 0)

    proj = mxu(att_ref[...], w_proj_ref[...], NN)
    centre = proj - jnp.mean(proj, -1, keepdims=True)
    inv_std = lax.rsqrt(jnp.mean(centre * centre, -1, keepdims=True) + EPS_NORM)
    normed = centre * inv_std
    upstream = grad_ref[...].astype(jnp.float32)
    d_gain_ref[...] = jnp.sum(upstream * normed, 0, keepdims=True)
    scaled = upstream * gain_ref[...]
    d_proj = inv_std * (
        scaled
        - jnp.mean(scaled, -1, keepdims=True)
        - normed * jnp.mean(scaled * normed, -1, keepdims=True)
    )
    d_proj = d_proj.astype(jnp.bfloat16)
    d_wproj_ref[...] = mxu(att_ref[...], d_proj, TN)
    d_att_ref[...] = mxu(d_proj, w_proj_ref[...], NT).astype(jnp.bfloat16)
    d_bias_ref[...] = jnp.zeros_like(d_bias_ref)
    d_cos_ref[...] = jnp.zeros_like(d_cos_ref)

    def backward(w, carry):
        rows = pl.ds(pl.multiple_of(w * length, length), length)
        for g in range(groups):
            query, key, value = load(w, g, 0), load(w, g, 1), load(w, g, 2)
            d_att = d_att_ref[rows, g * lanes : (g + 1) * lanes]
            probs = probs_ref[w, g]
            cosine = cos_ref[w, g]
            tall = spread(key, head_dim, length)
            d_probs = mxu(d_att, spread(value, head_dim, length), NT)
            d_value = gather_heads(
                mxu(probs.astype(jnp.bfloat16), d_att, TN), head_dim, length
            )
            d_scores = probs * (d_probs - mxu_fine(d_probs * probs, wide_ones, NN))
            d_bias_ref[g] += d_scores
            d_cos_ref[g] += d_scores * cosine
            scaled_scores = d_scores * scale_ref[g]
            query32, key32 = query.astype(jnp.float32), key.astype(jnp.float32)
            query_sum = mxu_fine(jnp.square(query32), lane_ones, NN)
            query_wide = lax.rsqrt(query_sum + 1.0)
            query_inv = lax.rsqrt(mxu_fine(jnp.square(query32), lane_lane, NN) + 1.0)
            key_inv = lax.rsqrt(mxu_fine(jnp.square(key32), lane_lane, NN) + 1.0)
            d_unit_q = mxu((scaled_scores * key_row_inv(tall)).astype(jnp.bfloat16), tall, NN)
            d_unit_k = gather_heads(
                mxu((scaled_scores * query_wide).astype(jnp.bfloat16), query, TN), head_dim, length
            )
            unit_q, unit_k = query32 * query_inv, key32 * key_inv
            d_query = query_inv * (d_unit_q - unit_q * mxu_fine(unit_q * d_unit_q, lane_lane, NN))
            d_key = key_inv * (d_unit_k - unit_k * mxu_fine(unit_k * d_unit_k, lane_lane, NN))
            for part, grad in enumerate((d_query, d_key, d_value)):
                d_qkv_ref[rows, part * depth + g * lanes : part * depth + (g + 1) * lanes] = (
                    grad.astype(jnp.bfloat16)
                )
        return carry

    lax.fori_loop(0, count, backward, 0)
    d_wqkv_ref[...] = mxu(flat_ref[...], d_qkv_ref[...], TN)
    d_flat_ref[...] = mxu(d_qkv_ref[...], w_qkv_ref[...], NT).astype(jnp.bfloat16)


def offset_onehot(window):
    places = np.arange(window * window)
    row_of, col_of = places // window, places % window
    offset = (row_of[:, None] - row_of[None, :] + window - 1) * (2 * window - 1) + (
        col_of[:, None] - col_of[None, :] + window - 1
    )
    return jnp.asarray(offset.reshape(-1), jnp.int32)


def three_parts(value):
    high = lax.reduce_precision(value, 8, 7)
    middle = lax.reduce_precision(value - high, 8, 7)
    return jnp.concatenate([high, middle, value - high - middle], 0).astype(jnp.bfloat16)


def local_grads(block, grad_block, row_base, col_base, height, width, window, params):
    w_qkv, w_proj, table_logits, logit_scale, gain = params
    images, rows, cols, depth = block.shape
    heads = logit_scale.shape[0]
    length = window * window
    groups = heads // GROUP
    wide = GROUP * length
    flat = to_windows(block, window).reshape(-1, depth)
    grad_flat = to_windows(grad_block, window).reshape(-1, depth)
    tokens = flat.shape[0]
    count = tokens // length
    scale = jnp.exp(jnp.minimum(logit_scale, SCALE_CAP))
    scale_rows = jnp.repeat(scale.reshape(groups, GROUP), length, 1).reshape(groups, 1, wide)
    sigma = jax.nn.sigmoid(table_logits)
    entries = table_logits.shape[1]
    hot = offset_onehot(window)[None, :] == jnp.arange(entries, dtype=jnp.int32)[:, None]
    hot = hot.astype(jnp.bfloat16)
    parts = jnp.dot(three_parts(sigma * BIAS_RANGE), hot, preferred_element_type=jnp.float32)
    rel_bias = jnp.sum(parts.reshape(3, heads, -1), 0).reshape(groups, GROUP, length, length)
    rel_bias = rel_bias.transpose(0, 2, 1, 3).reshape(groups, length, wide)
    f32, b16 = jnp.float32, jnp.bfloat16
    d_flat, d_wqkv, d_wproj, d_bias, d_cos, d_gain = pl.pallas_call(
        functools.partial(local_kernel, cols // window, height, width, window),
        out_shape=[
            jax.ShapeDtypeStruct((tokens, depth), b16),
            jax.ShapeDtypeStruct((depth, 3 * depth), f32),
            jax.ShapeDtypeStruct((depth, depth), f32),
            jax.ShapeDtypeStruct((groups, length, wide), f32),
            jax.ShapeDtypeStruct((groups, length, wide), f32),
            jax.ShapeDtypeStruct((1, depth), f32),
        ],
        in_specs=[VMEM] * 7,
        out_specs=[VMEM] * 6,
        scratch_shapes=[
            pltpu.VMEM((tokens, 3 * depth), b16),
            pltpu.VMEM((tokens, depth), b16),
            pltpu.VMEM((tokens, depth), b16),
            pltpu.VMEM((tokens, 3 * depth), b16),
            pltpu.VMEM((count, groups, length, wide), f32),
            pltpu.VMEM((count, groups, length, wide), f32),
        ],
        compiler_params=pltpu.CompilerParams(vmem_limit_bytes=48 * 2**20),
        cost_estimate=pl.CostEstimate(
            flops=4_000_000_000, bytes_accessed=8_000_000, transcendentals=400_000
        ),
        name="local_grads",
    )(flat, grad_flat, w_qkv, w_proj, rel_bias, scale_rows, gain.reshape(1, depth))
    heads_bias = d_bias.reshape(groups, length, GROUP, length).transpose(0, 2, 1, 3)
    heads_bias = heads_bias.reshape(heads, length * length)
    sums = lax.dot_general(three_parts(heads_bias), hot, NT, preferred_element_type=jnp.float32)
    d_table = jnp.sum(sums.reshape(3, heads, entries), 0) * (BIAS_RANGE * sigma * (1.0 - sigma))
    live = (logit_scale < SCALE_CAP).astype(jnp.float32)
    d_scale = jnp.sum(d_cos.reshape(groups, length, GROUP, length), (1, 3)).reshape(heads)
    d_scale = d_scale * scale * live
    d_block = from_windows(d_flat.reshape(images, count, length, depth), images, rows, cols, window)
    return (d_block, (d_wqkv, d_wproj, d_table, d_scale, d_gain.reshape(depth)))


def reduce_kernel(
    shape, wqkv_ref, wproj_ref, small_ref, qkv_out, proj_out, small_out,
    core_send, core_get, image_keep, image_send, image_get, near_send, near_get, own, whole, core_all,
    small_core, small_image, small_a, small_b, small_near,
    core_sems, image_sems, near_sems, all_sems, last_sems, tiny_sems,
):
    size_h, size_w = shape
    chips = size_h // 2
    peers = chips * size_w
    ha, wa, ba = lax.axis_index("ha"), lax.axis_index("wa"), lax.axis_index("ba")
    core = ha % 2
    me = wa * chips + ha // 2
    partner = (ha + 1 - 2 * core, wa, ba)
    image = (ha, wa, 1 - ba)

    def peer(step):
        other = lax.rem(me + step, peers)
        return other, (other % chips * 2 + core, other // chips, ba)

    barrier = pltpu.get_barrier_semaphore()
    pl.semaphore_signal(barrier, inc=1, device_id=partner, device_id_type=MESH)
    pl.semaphore_signal(barrier, inc=1, device_id=image, device_id_type=MESH)
    for step in range(1, peers):
        pl.semaphore_signal(barrier, inc=1, device_id=peer(step)[1], device_id_type=MESH)

    depth = wqkv_ref.shape[0]
    half = depth // 2
    q_half, p_half = wqkv_ref.shape[1] // 2, wproj_ref.shape[1] // 2
    f32, b16 = jnp.float32, jnp.bfloat16
    mine = pl.ds(pl.multiple_of(core * half, 16), half)
    theirs = pl.ds(pl.multiple_of((1 - core) * half, 16), half)
    core_send[:, : 2 * q_half] = wqkv_ref[theirs, :].astype(b16)
    core_send[:, 2 * q_half :] = wproj_ref[theirs, :].astype(b16)
    pl.semaphore_wait(barrier, peers + 1)

    def start(src, dst, sems, device):
        copy = pltpu.make_async_remote_copy(
            src_ref=src, dst_ref=dst, send_sem=sems.at[0], recv_sem=sems.at[1],
            device_id=device, device_id_type=MESH,
        )
        copy.start()
        return copy

    big = start(core_send, core_get, core_sems, partner)
    tiny = start(small_ref, small_core, tiny_sems.at[0], partner)
    tiny.wait()
    small_a[...] = small_ref[...] + small_core[...]
    tiny = start(small_a, small_image, tiny_sems.at[1], image)
    big.wait()

    def halves(first):
        q = wqkv_ref[mine, first * q_half : (first + 1) * q_half]
        p = wproj_ref[mine, first * p_half : (first + 1) * p_half]
        gq = core_get[:, first * q_half : (first + 1) * q_half]
        gp = core_get[:, 2 * q_half + first * p_half : 2 * q_half + (first + 1) * p_half]
        return q + gq.astype(f32), p + gp.astype(f32)

    low, high = halves(0), halves(1)
    for part, (a, b) in enumerate(zip(low, high)):
        place = slice(0, q_half) if part == 0 else slice(q_half, q_half + p_half)
        image_send[:, place] = jnp.where(ba == 0, b, a).astype(b16)
        image_keep[:, place] = jnp.where(ba == 0, a, b)
    big = start(image_send, image_get, image_sems, image)
    tiny.wait()
    small_b[...] = small_a[...] + small_image[...]
    tinies = []
    for step in range(1, peers):
        tinies.append(start(small_b, small_near.at[step - 1], tiny_sems.at[step + 1], peer(step)[1]))
    big.wait()
    total = image_keep[...] + image_get[...].astype(f32)
    r, c = near_send.shape[1:]
    split_c = total.shape[1] // c
    for j in range(peers):
        row, col = j // split_c * r, j % split_c * c
        near_send[j] = total[row : row + r, col : col + c].astype(b16)
    copies = []
    for step in range(1, peers):
        other, device = peer(step)
        copies.append(start(near_send.at[other], near_get.at[step - 1], near_sems.at[step - 1], device))
    for copy in tinies:
        copy.wait()
    small = small_b[...]
    for step in range(1, peers):
        small = small + small_near[step - 1]
    small_out[...] = small
    for copy in copies:
        copy.wait()
    total = near_send[me].astype(f32)
    for step in range(1, peers):
        total = total + near_get[step - 1].astype(f32)
    own[...] = total.astype(b16)
    whole[me] = own[...]
    copies = []
    for step in range(1, peers):
        _, device = peer(step)
        copies.append(start(own, whole.at[me], all_sems.at[step - 1], device))
    for copy in copies:
        copy.wait()
    last = start(whole, core_all, last_sems, partner)

    def put(source, first):
        for j in range(peers):
            row, col = j // split_c * r, j % split_c * c
            block = source[j].astype(f32)
            rows = pl.ds(pl.multiple_of(first * half + row, 8), r)
            q_part = max(0, min(c, q_half - col))
            if q_part > 0:
                qkv_out[rows, col : col + q_part] = block[:, :q_part]
            if q_part < c:
                begin = col + q_part - q_half
                proj_out[rows, begin : begin + c - q_part] = block[:, q_part:]

    put(whole, core)
    last.wait()
    put(core_all, 1 - core)


def reduce_all(d_wqkv, d_wproj, small):
    size_h, size_w = lax.axis_size("ha"), lax.axis_size("wa")
    peers = size_h // 2 * size_w
    depth = d_wqkv.shape[0]
    half = depth // 2
    cols = (d_wqkv.shape[1] + d_wproj.shape[1]) // 2
    split_c = 2
    r, c = half * split_c // peers, cols // split_c
    f32, b16 = jnp.float32, jnp.bfloat16
    tiny = small.shape
    return pl.pallas_call(
        functools.partial(reduce_kernel, (size_h, size_w)),
        out_shape=[
            jax.ShapeDtypeStruct((depth, d_wqkv.shape[1] // 2), f32),
            jax.ShapeDtypeStruct((depth, d_wproj.shape[1] // 2), f32),
            jax.ShapeDtypeStruct(tiny, f32),
        ],
        in_specs=[VMEM] * 3,
        out_specs=[VMEM] * 3,
        scratch_shapes=[
            pltpu.VMEM((half, 2 * cols), b16),
            pltpu.VMEM((half, 2 * cols), b16),
            pltpu.VMEM((half, cols), f32),
            pltpu.VMEM((half, cols), b16),
            pltpu.VMEM((half, cols), b16),
            pltpu.VMEM((peers, r, c), b16),
            pltpu.VMEM((peers - 1, r, c), b16),
            pltpu.VMEM((r, c), b16),
            pltpu.VMEM((peers, r, c), b16),
            pltpu.VMEM((peers, r, c), b16),
            pltpu.VMEM(tiny, f32),
            pltpu.VMEM(tiny, f32),
            pltpu.VMEM(tiny, f32),
            pltpu.VMEM(tiny, f32),
            pltpu.VMEM((peers - 1, *tiny), f32),
            pltpu.SemaphoreType.DMA((2,)),
            pltpu.SemaphoreType.DMA((2,)),
            pltpu.SemaphoreType.DMA((peers - 1, 2)),
            pltpu.SemaphoreType.DMA((peers - 1, 2)),
            pltpu.SemaphoreType.DMA((2,)),
            pltpu.SemaphoreType.DMA((peers + 1, 2)),
        ],
        compiler_params=pltpu.CompilerParams(
            collective_id=0, has_side_effects=True, vmem_limit_bytes=48 * 2**20
        ),
        name="reduce_all",
    )(d_wqkv, d_wproj, small)


def can_reduce(d_wqkv):
    peers = lax.axis_size("ha") // 2 * lax.axis_size("wa")
    pairs = lax.axis_size("ha") % 2 == 0 and lax.axis_size("ba") == 2
    return pairs and peers > 1 and d_wqkv.shape[0] % peers == 0 and d_wqkv.shape[0] // peers % 16 == 0


def pack_small(d_table, d_scale, d_gain):
    heads, entries = d_table.shape
    lanes = -(-entries // 128) * 128
    flat = jnp.concatenate([d_scale, d_gain])
    rows = -(-flat.shape[0] // lanes)
    flat = jnp.pad(flat, (0, rows * lanes - flat.shape[0])).reshape(rows, lanes)
    table = jnp.pad(d_table, ((0, 0), (0, lanes - entries)))
    full = jnp.concatenate([table, flat], 0)
    return jnp.pad(full, ((0, -full.shape[0] % 8), (0, 0)))


def unpack_small(full, heads, entries, depth):
    flat = full[heads:].reshape(-1)
    return full[:heads, :entries], flat[:heads], flat[heads : heads + depth]


def shift_in(tokens, cotangent, shift):
    stacked = jnp.stack([tokens, cotangent])
    below = from_behind(stacked[:, :, :shift], "ha", -1)
    tall = jnp.concatenate([stacked[:, :, shift:], below], 2)
    beside = from_behind(tall[:, :, :, :shift], "wa", -1)
    moved = jnp.concatenate([tall[:, :, :, shift:], beside], 3)
    return (moved[0], moved[1])


def shift_out(grads, shift):
    rows = grads.shape[1]
    cols = grads.shape[2]
    right = from_behind(grads[:, :, cols - shift :], "wa", 1)
    wide = jnp.concatenate([right, grads[:, :, : cols - shift]], 2)
    lower = from_behind(wide[:, rows - shift :], "ha", 1)
    return jnp.concatenate([lower, wide[:, : rows - shift]], 1)


def shards(tokens, cotangent, w_qkv, w_proj, table_logits, logit_scale, gain):
    rows = tokens.shape[1]
    cols = tokens.shape[2]
    shift = WIN // 2
    height = rows * lax.axis_size("ha")
    width = cols * lax.axis_size("wa")
    row_base = lax.axis_index("ha") * rows
    col_base = lax.axis_index("wa") * cols
    params = (w_qkv, w_proj, table_logits, logit_scale, gain)
    moved, moved_grad = shift_in(tokens, cotangent, shift)
    d_moved, parts = local_grads(moved, moved_grad, row_base, col_base, height, width, WIN, params)
    back = shift_out(d_moved, shift)
    d_tokens = (cotangent.astype(jnp.float32) + back.astype(jnp.float32)).astype(jnp.bfloat16)
    d_wqkv, d_wproj, d_table, d_scale, d_gain = parts
    if can_reduce(d_wqkv):
        small = pack_small(d_table, d_scale, d_gain)
        half_qkv, half_proj, small = reduce_all(d_wqkv, d_wproj, small)
        d_table, d_scale, d_gain = unpack_small(small, *d_table.shape, d_gain.shape[0])
    else:
        half_qkv, half_proj = (
            lax.psum_scatter(d_wqkv.astype(jnp.bfloat16), "ba", scatter_dimension=1, tiled=True).astype(
                jnp.float32
            ),
            lax.psum_scatter(
                d_wproj.astype(jnp.bfloat16), "ba", scatter_dimension=1, tiled=True
            ).astype(jnp.float32),
        )
        half_qkv, half_proj = lax.psum((half_qkv, half_proj), ("ha", "wa"))
        d_table, d_scale, d_gain = lax.psum((d_table, d_scale, d_gain), ("ha", "wa", "ba"))
    return (d_tokens, half_qkv, half_proj, d_table, d_scale, d_gain)


def solution(mesh):
    return jax.shard_map(
        shards,
        mesh=mesh,
        in_specs=(P("ba", "ha", "wa", None), P("ba", "ha", "wa", None), P(), P(), P(), P(), P()),
        out_specs=(P("ba", "ha", "wa", None), P(None, "ba"), P(None, "ba"), P(), P(), P()),
        check_vma=False,
    )
```
